32 devices in a mesh: row: 4 (over y, core), col: 8 (over z, x).
Axes of the slice: x: 2, y: 2, z: 4, core: 2. Of those that a mesh axis runs over, the one named last changes fastest.
Arguments:
- singles: bfloat16 [96, 384], P(('row', 'col')), may hold values from -6 to 6
- pair: float32 [96, 96, 128], P('row', 'col'), may hold values from -48 to 48
- frames: float32 [96, 12], P(('row', 'col')), may hold values from -9 to 9, as said below
- w_query: bfloat16 [384, 336], replicated, may hold values from -0.3125 to 0.3125
- w_keyval: bfloat16 [384, 816], replicated, may hold values from -0.3125 to 0.3125
- w_bias: float32 [128, 12], replicated, may hold values from -1 to 1
- head_weights: float32 [12], replicated, may hold values from -2 to 1
- w_out: bfloat16 [2112, 384], replicated, may hold values from -0.125 to 0.125
Outputs:
- update: float32 [96, 384], P(('row', 'col'))
The draws below stay inside these ranges and needn't reach their ends.
Inputs may be any that keep to these rules, and one draw needn't show every extreme that they name: `frames`: the first nine entries of a row are a rotation matrix in row-major order, the last three a translation.
All inputs are finite; a program needn't handle non-finite values.
Results may differ from the reference program's by a relative error of at most 0.0029.
Values sent between devices are 32-bit elements; how exact they have to be, the bound alone decides.
A program may use at most 64 MiB of HBM per device.

```python
import math
import jax
import jax.numpy as jnp
from jax import lax

CS = 384
CZ = 128
H = 12
CH = 16
PQ = 4
PV = 8
RESIDUES = 96


def sign_vector(key):
    coin_flips = jax.random.bernoulli(jax.random.fold_in(key, 101), 0.5, (CZ,))
    return jnp.where(coin_flips, 1.0, -1.0).astype(jnp.float32)


def draw_pair(key, part):
    base_key = jax.random.fold_in(key, 202)
    shape_all = (RESIDUES, RESIDUES, CZ)
    values = jnp.clip(jax.random.normal(base_key, shape_all, jnp.float32), -6.0, 6.0)
    return values.astype(jnp.float32)


def draw_w_bias(key, part):
    signs_cz = sign_vector(key)
    normal_part = jax.random.normal(jax.random.fold_in(key, 404), (CZ, H), jnp.float32)
    magnitude = jnp.minimum(jnp.abs(normal_part), 4.0)
    return (signs_cz[:, None] * magnitude / jnp.sqrt(jnp.float32(CZ))).astype(jnp.float32)


def draw_frames(key, part):
    quaternion = jax.random.normal(jax.random.fold_in(key, 505), (RESIDUES, 4), jnp.float32)
    comp_w = jnp.abs(quaternion[:, 0]) + 1.0
    comp_x = quaternion[:, 1]
    comp_y = quaternion[:, 2]
    comp_z = quaternion[:, 3]
    norm_sq = comp_w * comp_w + comp_x * comp_x + comp_y * comp_y + comp_z * comp_z
    scale_inv = 1.0 / jnp.sqrt(norm_sq)
    comp_w = comp_w * scale_inv
    comp_x = comp_x * scale_inv
    comp_y = comp_y * scale_inv
    comp_z = comp_z * scale_inv
    rotation = jnp.stack([1.0 - 2.0 * (comp_y * comp_y + comp_z * comp_z), 2.0 * (comp_x * comp_y - comp_w * comp_z), 2.0 * (comp_x * comp_z + comp_w * comp_y), 2.0 * (comp_x * comp_y + comp_w * comp_z), 1.0 - 2.0 * (comp_x * comp_x + comp_z * comp_z), 2.0 * (comp_y * comp_z - comp_w * comp_x), 2.0 * (comp_x * comp_z - comp_w * comp_y), 2.0 * (comp_y * comp_z + comp_w * comp_x), 1.0 - 2.0 * (comp_x * comp_x + comp_y * comp_y)], axis=1)
    trans_key = jax.random.fold_in(key, 606)
    shift = jnp.clip(1.5 * jax.random.normal(trans_key, (RESIDUES, 3), jnp.float32), -9.0, 9.0)
    return jnp.concatenate([rotation, shift], 1).astype(jnp.float32)


def shard_levels(own_key, extent, cuts, smallest, top_value):
    gain = 1.0
    for dim, parts in cuts:
        steps = jax.random.uniform(jax.random.fold_in(jax.random.fold_in(own_key, 6), dim), (parts,), jnp.float32, smallest / len(cuts), top_value / len(cuts))
        gain = gain * jnp.repeat(jnp.exp(steps), extent[dim] // parts).reshape((-1,) + (1,) * (len(extent) - 1 - dim))
    return gain


def normal_values(key, extent, deviation, reach, pieces=(), dtype=jnp.bfloat16):
    gain = shard_levels(key, extent, pieces, -0.22, 0.18) if pieces else 1.0
    result = jax.random.normal(key, extent, jnp.float32) * deviation * gain
    return jnp.minimum(jnp.maximum(result, -reach), reach).astype(dtype)


def setup_inputs(seed: int = 0) -> dict:
    streams_of = jax.random.split(jax.random.key(seed), 9)
    singles = normal_values(streams_of[0], (RESIDUES, CS), 1.0, 6.0, ((0, 32),))
    pair = draw_pair(jax.random.fold_in(streams_of[8], 71), 0)
    frames = draw_frames(jax.random.fold_in(streams_of[8], 71), 0)
    w_query = normal_values(streams_of[3], (CS, H * CH + 3 * H * PQ), CS ** -0.5, 0.3125)
    w_keyval = normal_values(streams_of[4], (CS, 2 * H * CH + 3 * H * (PQ + PV)), CS ** -0.5, 0.3125)
    w_bias = draw_w_bias(jax.random.fold_in(streams_of[8], 71), 0)
    head_weights = jnp.clip(jax.random.uniform(streams_of[6], (H,), jnp.float32, -2.0, 1.0), -2.0, 1.0)
    w_out = normal_values(streams_of[7], (H * (CH + 4 * PV + CZ), CS), (H * (CH + 4 * PV + CZ)) ** -0.5, 0.125)
    return dict(singles=singles, pair=pair, frames=frames, w_query=w_query, w_keyval=w_keyval, w_bias=w_bias, head_weights=head_weights, w_out=w_out)


HIGHEST = lax.Precision.HIGHEST

def rigid_apply(frames, points):
    rotation = frames[:, :9].reshape(frames.shape[0], 3, 3)
    moved = jnp.einsum('nab,nbm->nam', rotation, points, precision=HIGHEST)
    return moved + frames[:, 9:12, None]

def query_side(singles, frames, w_query):
    row_count = singles.shape[0]
    scalar_width = H * CH
    projected = jnp.dot(singles, w_query, preferred_element_type=jnp.float32)
    points = rigid_apply(frames, projected[:, scalar_width:].reshape(row_count, 3, H * PQ))
    return jnp.concatenate([projected[:, :scalar_width], points.reshape(row_count, 3 * H * PQ)], 1)

def key_side(singles, frames, w_keyval):
    row_count = singles.shape[0]
    scalar_width = 2 * H * CH
    point_end = scalar_width + 3 * H * PQ
    projected = jnp.dot(singles, w_keyval, preferred_element_type=jnp.float32)
    key_points = rigid_apply(frames, projected[:, scalar_width:point_end].reshape(row_count, 3, H * PQ))
    value_points = rigid_apply(frames, projected[:, point_end:].reshape(row_count, 3, H * PV))
    return jnp.concatenate([projected[:, :scalar_width], key_points.reshape(row_count, 3 * H * PQ), value_points.reshape(row_count, 3 * H * PV)], 1)

def logits_of(query_feat, key_feat, pair_block, w_bias, head_weights):
    query_rows = query_feat.shape[0]
    key_rows = key_feat.shape[0]
    scalar_width = H * CH
    query_vec = query_feat[:, :scalar_width].reshape(query_rows, H, CH)
    query_points = query_feat[:, scalar_width:].reshape(query_rows, 3, H, PQ)
    key_vec = key_feat[:, :scalar_width].reshape(key_rows, H, CH)
    key_points = key_feat[:, 2 * scalar_width:2 * scalar_width + 3 * H * PQ].reshape(key_rows, 3, H, PQ)
    scalar = jnp.einsum('ihc,jhc->ihj', query_vec, key_vec, precision=HIGHEST) / math.sqrt(CH)
    pair_bias = jnp.einsum('ijc,ch->ihj', pair_block, w_bias, precision=HIGHEST)
    cross_term = jnp.einsum('iahp,jahp->ihj', query_points, key_points, precision=HIGHEST)
    query_square = lax.optimization_barrier(jnp.sum(query_points * query_points, axis=(1, 3)))
    key_square = lax.optimization_barrier(jnp.sum(key_points * key_points, axis=(1, 3)))
    distance = query_square[:, :, None] + key_square.T[None, :, :] - 2.0 * cross_term
    weight = jax.nn.softplus(head_weights) * (math.sqrt(2.0 / (9.0 * PQ)) / 2.0)
    return math.sqrt(1.0 / 3.0) * (scalar + pair_bias - weight[None, :, None] * distance)

def weighted(exponent, key_feat, pair_block):
    key_rows = key_feat.shape[0]
    scalar_width = H * CH
    value_vec = key_feat[:, scalar_width:2 * scalar_width].reshape(key_rows, H, CH)
    value_points = key_feat[:, 2 * scalar_width + 3 * H * PQ:].reshape(key_rows, 3, H, PV)
    weight_sum = lax.optimization_barrier(jnp.sum(exponent, axis=2))
    scalar = jnp.einsum('ihj,jhc->ihc', exponent, value_vec, precision=HIGHEST)
    points = jnp.einsum('ihj,jahp->iahp', exponent, value_points, precision=HIGHEST)
    paired = jnp.einsum('ihj,ijc->ihc', exponent, pair_block, precision=HIGHEST)
    return (weight_sum, scalar, points, paired)

def finish_rest(scalar, points, frames, w_out):
    row_count = scalar.shape[0]
    rotation = frames[:, :9].reshape(row_count, 3, 3)
    relative = points - frames[:, 9:12, None, None]
    local_points = jnp.einsum('nba,nbhp->nahp', rotation, relative, precision=HIGHEST)
    length = jnp.sqrt(lax.optimization_barrier(jnp.sum(local_points * local_points, axis=1)) + 1.0)
    features = jnp.concatenate([scalar.reshape(row_count, H * CH), local_points.reshape(row_count, 3 * H * PV), length.reshape(row_count, H * PV)], 1)
    features = features.astype(jnp.bfloat16)
    return jnp.dot(features, w_out[:H * (CH + 4 * PV)], preferred_element_type=jnp.float32)

def paired_term(paired, w_out):
    row_count = paired.shape[0]
    pair_rows = w_out[H * (CH + 4 * PV):].astype(jnp.float32)
    return jnp.dot(paired.reshape(row_count, H * CZ), pair_rows, precision=HIGHEST)

def finish(weight_sum, scalar, points, paired, frames, w_out):
    scalar = scalar / weight_sum[:, :, None]
    points = points / weight_sum[:, None, :, None]
    paired = paired / weight_sum[:, :, None]
    return finish_rest(scalar, points, frames, w_out) + paired_term(paired, w_out)

def reference(singles, pair, frames, w_query, w_keyval, w_bias, head_weights, w_out):
    query_feat = query_side(singles, frames, w_query)
    key_feat = key_side(singles, frames, w_keyval)
    residues = singles.shape[0]
    block_rows = 128 if residues % 128 == 0 else residues

    def one_block(first_row):
        query_part = lax.dynamic_slice_in_dim(query_feat, first_row, block_rows, 0)
        pair_part = lax.dynamic_slice_in_dim(pair, first_row, block_rows, 0)
        frame_part = lax.dynamic_slice_in_dim(frames, first_row, block_rows, 0)
        logits = logits_of(query_part, key_feat, pair_part, w_bias, head_weights)
        exponent = jnp.exp(logits - lax.optimization_barrier(jnp.max(logits, axis=2, keepdims=True)))
        weight_sum, scalar, points, paired = weighted(exponent, key_feat, pair_part)
        return finish(weight_sum, scalar, points, paired, frame_part, w_out)
    starts = (jnp.arange(residues // block_rows) * block_rows).astype(jnp.int32)
    blocks = lax.map(one_block, starts)
    return blocks.reshape(residues, CS)
```

```python
import functools
import math

import jax
import jax.numpy as jnp
from jax import lax
from jax.experimental import pallas as pl
from jax.experimental.pallas import tpu as pltpu
from jax.sharding import PartitionSpec as P

CS = 384
CZ = 128
H = 12
CH = 16
PQ = 4
PV = 8

HP = 16
LANES = 128
HIGHEST = lax.Precision.HIGHEST
MESH = pl.DeviceIdType.MESH
NT = (((1,), (1,)), ((), ()))
NN = (((1,), (0,)), ((), ()))


def round_up(value, step):
    return (value + step - 1) // step * step


def dot_exact(left, right, dims):
    return lax.dot_general(
        left, right, dims, precision=HIGHEST, preferred_element_type=jnp.float32
    )


def head_mask(width, offset, per_head, heads_period):
    feature = lax.broadcasted_iota(jnp.int32, (HP, width), 1) - offset
    head = lax.broadcasted_iota(jnp.int32, (HP, width), 0)
    return (feature % heads_period) // per_head == head


def moved_points(frame, local, width):
    parts = [local[:, b * width : (b + 1) * width] for b in range(3)]
    return [
        frame[:, 3 * a : 3 * a + 1] * parts[0]
        + frame[:, 3 * a + 1 : 3 * a + 2] * parts[1]
        + frame[:, 3 * a + 2 : 3 * a + 3] * parts[2]
        + frame[:, 9 + a : 10 + a]
        for a in range(3)
    ]


def kernel(
    sizes,
    singles_ref,
    frames_ref,
    w_bias_ref,
    heads_ref,
    pair_hbm,
    w_query_hbm,
    w_keyval_hbm,
    w_out_hbm,
    out_ref,
    x_all,
    pair_own,
    pair_all,
    w_query_ref,
    w_keyval_ref,
    w_out_ref,
    k_feat,
    v_feat,
    load_sem,
    x_send,
    x_recv,
    p_send,
    p_recv,
):
    row_devs, col_devs = sizes
    devices = row_devs * col_devs
    rows = singles_ref.shape[0]
    keys = pair_own.shape[1]
    key_pad = round_up(keys, 8)
    slots = col_devs * key_pad
    row = lax.axis_index("row")
    col = lax.axis_index("col")
    me = row * col_devs + col
    own_rows = pl.ds(col * rows, rows)

    loads = [
        pltpu.make_async_copy(pair_hbm, pair_own, load_sem.at[0]),
        pltpu.make_async_copy(pair_hbm.at[own_rows], pair_all.at[:, col], load_sem.at[1]),
        pltpu.make_async_copy(w_query_hbm, w_query_ref, load_sem.at[2]),
        pltpu.make_async_copy(w_keyval_hbm, w_keyval_ref, load_sem.at[3]),
        pltpu.make_async_copy(w_out_hbm, w_out_ref, load_sem.at[4]),
    ]
    for load in loads:
        load.start()

    barrier = pltpu.get_barrier_semaphore()

    def greet(step, carry):
        peer = lax.rem(me + step, devices)
        pl.semaphore_signal(
            barrier,
            inc=1,
            device_id=(peer // col_devs, lax.rem(peer, col_devs)),
            device_id_type=MESH,
        )
        return carry

    lax.fori_loop(1, devices, greet, 0)

    def slot_of(device):
        first = device * rows
        return first // keys * key_pad + lax.rem(first, keys)

    for c in range(col_devs):
        for slot in range(c * key_pad + keys, (c + 1) * key_pad):
            x_all[slot] = jnp.zeros(x_all.shape[1:], jnp.float32)
    single = singles_ref[...]
    frame = frames_ref[...]
    own_slot = pl.ds(slot_of(me), rows)
    for t in range(CS // LANES):
        x_all[own_slot, t, :] = single[:, t * LANES : (t + 1) * LANES].astype(jnp.float32)
    x_all[own_slot, CS // LANES, :] = jnp.concatenate(
        [frame, jnp.zeros((rows, LANES - 12), jnp.float32)], 1
    )
    loads[0].wait()
    pl.semaphore_wait(barrier, devices - 1)

    def x_copy(slot_device, peer, send_index, recv_index):
        slot = pl.ds(slot_of(slot_device), rows)
        return pltpu.make_async_remote_copy(
            src_ref=x_all.at[slot],
            dst_ref=x_all.at[slot],
            send_sem=x_send.at[send_index],
            recv_sem=x_recv.at[recv_index],
            device_id=(peer // col_devs, lax.rem(peer, col_devs)),
            device_id_type=MESH,
        )

    def p_copy(peer_col, sent_col, send_index, recv_index):
        return pltpu.make_async_remote_copy(
            src_ref=pair_own.at[pl.ds(peer_col * rows, rows)],
            dst_ref=pair_all.at[:, sent_col],
            send_sem=p_send.at[send_index],
            recv_sem=p_recv.at[recv_index],
            device_id=(row, peer_col),
            device_id_type=MESH,
        )

    def send_x(step, carry):
        x_copy(me, lax.rem(me + step, devices), step, me).start()
        return carry

    def send_p(step, carry):
        p_copy(lax.rem(col + step, col_devs), col, step, col).start()
        return carry

    lax.fori_loop(1, devices, send_x, 0)
    lax.fori_loop(1, col_devs, send_p, 0)

    scalar = H * CH
    loads[2].wait()
    projected = jnp.dot(single, w_query_ref[...], preferred_element_type=jnp.float32)
    q_points = moved_points(frame, projected[:, scalar:], H * PQ)
    q_feat = jnp.concatenate([projected[:, :scalar]] + q_points, 1)

    raw = heads_ref[...]
    gamma_row = jnp.maximum(raw, 0.0) + jnp.log(1.0 + jnp.exp(-jnp.abs(raw)))
    eye = lax.broadcasted_iota(jnp.int32, (HP, H), 0) == lax.broadcasted_iota(
        jnp.int32, (HP, H), 1
    )
    gamma = jnp.sum(jnp.where(eye, gamma_row, 0.0), axis=1, keepdims=True)
    weight = gamma * (math.sqrt(2.0 / (9.0 * PQ)) / 2.0)
    scalar_part = jnp.where(head_mask(scalar, 0, CH, scalar), 1.0 / math.sqrt(CH), 0.0)
    point_mask = head_mask(3 * H * PQ, 0, PQ, H * PQ)
    point_part = jnp.where(point_mask, 2.0 * weight, 0.0)
    square_part = jnp.where(point_mask, -weight, 0.0)
    q_scale = jnp.concatenate([scalar_part, point_part], 1)
    spread = jnp.concatenate(
        [
            jnp.concatenate([q_feat[i : i + 1] * q_scale, square_part], 1)
            for i in range(rows)
        ],
        0,
    )
    q_square = [
        jnp.sum(
            jnp.where(point_mask, q_feat[i : i + 1, scalar:] ** 2, 0.0), axis=1, keepdims=True
        )
        * weight
        for i in range(rows)
    ]
    bias_weights = w_bias_ref[...]

    def wait_x(step, carry):
        source = lax.rem(me + devices - step, devices)
        x_copy(source, source, step, source).wait_recv()
        return carry

    lax.fori_loop(1, devices, wait_x, 0)
    loads[3].wait()

    chunk = LANES if slots % LANES == 0 else slots

    def key_side(start):
        part = pl.ds(start, chunk)
        inputs = [x_all[part, t, :].astype(jnp.bfloat16) for t in range(CS // LANES)]
        held = x_all[part, CS // LANES, :]
        values = jnp.dot(
            jnp.concatenate(inputs, 1), w_keyval_ref[...], preferred_element_type=jnp.float32
        )
        key_end = 2 * scalar + 3 * H * PQ
        key_points = moved_points(held, values[:, 2 * scalar : key_end], H * PQ)
        value_points = moved_points(held, values[:, key_end:], H * PV)
        squares = [point * point for point in key_points]
        k_feat[part, :] = jnp.concatenate([values[:, :scalar]] + key_points + squares, 1)
        v_feat[part, :] = jnp.concatenate([values[:, scalar : 2 * scalar]] + value_points, 1)

    if chunk == slots:
        key_side(0)
    else:

        @pl.loop(0, slots // chunk)
        def _(index):
            key_side(pl.multiple_of(index * chunk, chunk))

    inner = dot_exact(spread, k_feat[...], NT)

    def wait_p(step, carry):
        source = lax.rem(col + col_devs - step, col_devs)
        p_copy(source, source, step, source).wait_recv()
        return carry

    loads[1].wait()
    lax.fori_loop(1, col_devs, wait_p, 0)

    place = lax.rem(lax.broadcasted_iota(jnp.int32, (HP, slots), 1), key_pad)
    bias_rows = jnp.concatenate([bias_weights, jnp.zeros((CZ, HP - H), jnp.float32)], 1).T
    shares, pooled = [], []
    for i in range(rows):
        block = pair_all[i]
        if key_pad != keys:
            block = jnp.concatenate(
                [block, jnp.zeros((col_devs, key_pad - keys, CZ), jnp.float32)], 1
            )
        block = block.reshape(slots, CZ)
        bias = dot_exact(bias_rows, block, NT)
        logits = math.sqrt(1.0 / 3.0) * (inner[i * HP : (i + 1) * HP] + bias - q_square[i])
        if key_pad != keys:
            logits = jnp.where(place < keys, logits, -jnp.inf)
        exponent = jnp.exp(logits - jnp.max(logits, axis=1, keepdims=True))
        share = exponent / jnp.sum(exponent, axis=1, keepdims=True)
        shares.append(share)
        pooled.append(dot_exact(share, block, NN))

    gathered = dot_exact(jnp.concatenate(shares, 0), v_feat[...], NN)
    value_masks = [head_mask(scalar, 0, CH, scalar), head_mask(3 * H * PV, 0, PV, H * PV)]
    value_mask = jnp.concatenate([jnp.where(mask, 1.0, 0.0) for mask in value_masks], 1)
    kept = jnp.concatenate(
        [
            jnp.sum(
                gathered[i * HP : (i + 1) * HP] * value_mask,
                axis=0,
                keepdims=True,
            )
            for i in range(rows)
        ],
        0,
    )
    wide = H * PV
    relative = [
        kept[:, scalar + b * wide : scalar + (b + 1) * wide] - frame[:, 9 + b : 10 + b]
        for b in range(3)
    ]
    local = [
        frame[:, a : a + 1] * relative[0]
        + frame[:, 3 + a : 4 + a] * relative[1]
        + frame[:, 6 + a : 7 + a] * relative[2]
        for a in range(3)
    ]
    length = jnp.sqrt(local[0] ** 2 + local[1] ** 2 + local[2] ** 2 + 1.0)
    loads[4].wait()
    features = jnp.concatenate([kept[:, :scalar]] + local + [length], 1).astype(jnp.bfloat16)
    split = H * (CH + 4 * PV)
    total = jnp.dot(features, w_out_ref[0:split, :], preferred_element_type=jnp.float32)
    flat = jnp.concatenate(
        [
            jnp.concatenate([pooled[i][h : h + 1] for i in range(rows)], 0)
            for h in range(H)
        ],
        1,
    )
    high = flat.astype(jnp.bfloat16)
    rest = flat - high.astype(jnp.float32)
    middle = rest.astype(jnp.bfloat16)
    low = (rest - middle.astype(jnp.float32)).astype(jnp.bfloat16)
    w_pair = w_out_ref[split:, :]
    for piece in (low, middle, high):
        total = total + jnp.dot(piece, w_pair, preferred_element_type=jnp.float32)
    out_ref[...] = total

    def end_x(step, carry):
        peer = lax.rem(me + step, devices)
        x_copy(me, peer, step, me).wait_send()
        return carry

    def end_p(step, carry):
        p_copy(lax.rem(col + step, col_devs), col, step, col).wait_send()
        return carry

    lax.fori_loop(1, devices, end_x, 0)
    lax.fori_loop(1, col_devs, end_p, 0)


def solution(mesh):
    sizes = (mesh.shape["row"], mesh.shape["col"])
    devices = sizes[0] * sizes[1]

    def body(singles, pair, frames, w_query, w_keyval, w_bias, head_weights, w_out):
        rows = singles.shape[0]
        keys = pair.shape[1]
        slots = sizes[1] * round_up(keys, 8)
        vmem = pl.BlockSpec(memory_space=pltpu.VMEM)
        hbm = pl.BlockSpec(memory_space=pl.ANY)
        return pl.pallas_call(
            functools.partial(kernel, sizes),
            out_shape=jax.ShapeDtypeStruct((rows, w_out.shape[1]), jnp.float32),
            in_specs=[vmem] * 4 + [hbm] * 4,
            out_specs=vmem,
            scratch_shapes=[
                pltpu.VMEM((slots, CS // LANES + 1, LANES), jnp.float32),
                pltpu.VMEM(pair.shape, jnp.float32),
                pltpu.VMEM((rows, sizes[1], keys, CZ), jnp.float32),
                pltpu.VMEM(w_query.shape, w_query.dtype),
                pltpu.VMEM(w_keyval.shape, w_keyval.dtype),
                pltpu.VMEM(w_out.shape, w_out.dtype),
                pltpu.VMEM((slots, H * CH + 6 * H * PQ), jnp.float32),
                pltpu.VMEM((slots, H * CH + 3 * H * PV), jnp.float32),
                pltpu.SemaphoreType.DMA((5,)),
                pltpu.SemaphoreType.DMA((devices,)),
                pltpu.SemaphoreType.DMA((devices,)),
                pltpu.SemaphoreType.DMA((sizes[1],)),
                pltpu.SemaphoreType.DMA((sizes[1],)),
            ],
            compiler_params=pltpu.CompilerParams(
                collective_id=0, has_side_effects=True, vmem_limit_bytes=60 * 2**20
            ),
        )(
            singles,
            frames,
            w_bias,
            head_weights.reshape(1, H),
            pair,
            w_query,
            w_keyval,
            w_out,
        )

    return jax.shard_map(
        body,
        mesh=mesh,
        in_specs=(
            P(("row", "col"), None),
            P("row", "col", None),
            P(("row", "col"), None),
            P(),
            P(),
            P(),
            P(),
            P(),
        ),
        out_specs=P(("row", "col"), None),
        check_vma=False,
    )
```

```python
import functools
import math

import jax
import jax.numpy as jnp
from jax import lax
from jax.experimental import pallas as pl
from jax.experimental.pallas import tpu as pltpu
from jax.sharding import PartitionSpec as P

CS = 384
CZ = 128
H = 12
CH = 16
PQ = 4
PV = 8

HP = 16
LANES = 128
HIGHEST = lax.Precision.HIGHEST
MESH = pl.DeviceIdType.MESH
NT = (((1,), (1,)), ((), ()))
NN = (((1,), (0,)), ((), ()))


def round_up(value, step):
    return (value + step - 1) // step * step


def dot_exact(left, right, dims):
    return lax.dot_general(
        left, right, dims, precision=HIGHEST, preferred_element_type=jnp.float32
    )


def head_mask(width, offset, per_head, heads_period):
    feature = lax.broadcasted_iota(jnp.int32, (HP, width), 1) - offset
    head = lax.broadcasted_iota(jnp.int32, (HP, width), 0)
    return (feature % heads_period) // per_head == head


def moved_points(frame, local, width):
    parts = [local[:, b * width : (b + 1) * width] for b in range(3)]
    return [
        frame[:, 3 * a : 3 * a + 1] * parts[0]
        + frame[:, 3 * a + 1 : 3 * a + 2] * parts[1]
        + frame[:, 3 * a + 2 : 3 * a + 3] * parts[2]
        + frame[:, 9 + a : 10 + a]
        for a in range(3)
    ]


def moved_columns(frame, local, width):
    parts = [local[b * width : (b + 1) * width] for b in range(3)]
    return [
        frame[3 * a : 3 * a + 1] * parts[0]
        + frame[3 * a + 1 : 3 * a + 2] * parts[1]
        + frame[3 * a + 2 : 3 * a + 3] * parts[2]
        + frame[9 + a : 10 + a]
        for a in range(3)
    ]


def kernel(
    sizes,
    singles_ref,
    frames_ref,
    w_bias_ref,
    heads_ref,
    pair_hbm,
    w_query_hbm,
    w_keyval_hbm,
    w_out_hbm,
    out_ref,
    x_all,
    pair_raw,
    pair_own,
    pair_all,
    w_query_ref,
    w_keyval_ref,
    w_out_ref,
    k_feat,
    v_feat,
    load_sem,
    x_send,
    x_recv,
    p_send,
    p_recv,
):
    row_devs, col_devs = sizes
    devices = row_devs * col_devs
    rows = singles_ref.shape[0]
    keys = pair_own.shape[1]
    key_pad = round_up(keys, 8)
    slots = col_devs * key_pad
    row = lax.axis_index("row")
    col = lax.axis_index("col")
    me = row * col_devs + col

    loads = [
        pltpu.make_async_copy(pair_hbm, pair_raw, load_sem.at[0]),
        pltpu.make_async_copy(w_query_hbm, w_query_ref, load_sem.at[1]),
        pltpu.make_async_copy(w_keyval_hbm, w_keyval_ref, load_sem.at[2]),
        pltpu.make_async_copy(w_out_hbm, w_out_ref, load_sem.at[3]),
    ]
    for load in loads:
        load.start()

    barrier = pltpu.get_barrier_semaphore()

    def greet(step, carry):
        peer = lax.rem(me + step, devices)
        pl.semaphore_signal(
            barrier,
            inc=1,
            device_id=(peer // col_devs, lax.rem(peer, col_devs)),
            device_id_type=MESH,
        )
        return carry

    lax.fori_loop(1, devices, greet, 0)

    def slot_of(device):
        first = device * rows
        return first // keys * key_pad + lax.rem(first, keys)

    for c in range(col_devs):
        for slot in range(c * key_pad + keys, (c + 1) * key_pad):
            x_all[slot] = jnp.zeros(x_all.shape[1:], jnp.float32)
    single = singles_ref[...]
    frame = frames_ref[...]
    own_slot = pl.ds(slot_of(me), rows)
    for t in range(CS // LANES):
        x_all[own_slot, t, :] = single[:, t * LANES : (t + 1) * LANES].astype(jnp.float32)
    x_all[own_slot, CS // LANES, :] = jnp.concatenate(
        [frame, jnp.zeros((rows, LANES - 12), jnp.float32)], 1
    )
    loads[0].wait()
    for i in range(pair_own.shape[0]):
        pair_own[i] = pair_raw[:, i, :]
    for i in range(rows):
        pair_all[i, col] = pair_own[col * rows + i]
    pl.semaphore_wait(barrier, devices - 1)

    def x_copy(slot_device, peer, send_index, recv_index):
        slot = pl.ds(slot_of(slot_device), rows)
        return pltpu.make_async_remote_copy(
            src_ref=x_all.at[slot],
            dst_ref=x_all.at[slot],
            send_sem=x_send.at[send_index],
            recv_sem=x_recv.at[recv_index],
            device_id=(peer // col_devs, lax.rem(peer, col_devs)),
            device_id_type=MESH,
        )

    def p_copy(peer_col, sent_col, send_index, recv_index):
        return pltpu.make_async_remote_copy(
            src_ref=pair_own.at[pl.ds(peer_col * rows, rows)],
            dst_ref=pair_all.at[:, sent_col],
            send_sem=p_send.at[send_index],
            recv_sem=p_recv.at[recv_index],
            device_id=(row, peer_col),
            device_id_type=MESH,
        )

    def send_x(step, carry):
        x_copy(me, lax.rem(me + step, devices), step, me).start()
        return carry

    def send_p(step, carry):
        p_copy(lax.rem(col + step, col_devs), col, step, col).start()
        return carry

    lax.fori_loop(1, devices, send_x, 0)
    lax.fori_loop(1, col_devs, send_p, 0)

    scalar = H * CH
    loads[1].wait()
    projected = lax.dot_general(
        single, w_query_ref[...], NT, preferred_element_type=jnp.float32
    )
    q_points = moved_points(frame, projected[:, scalar:], H * PQ)
    q_feat = jnp.concatenate([projected[:, :scalar]] + q_points, 1)

    raw = heads_ref[...]
    gamma_row = jnp.maximum(raw, 0.0) + jnp.log(1.0 + jnp.exp(-jnp.abs(raw)))
    eye = lax.broadcasted_iota(jnp.int32, (HP, H), 0) == lax.broadcasted_iota(
        jnp.int32, (HP, H), 1
    )
    gamma = jnp.sum(jnp.where(eye, gamma_row, 0.0), axis=1, keepdims=True)
    weight = gamma * (math.sqrt(2.0 / (9.0 * PQ)) / 2.0)
    scalar_part = jnp.where(head_mask(scalar, 0, CH, scalar), 1.0 / math.sqrt(CH), 0.0)
    point_mask = head_mask(3 * H * PQ, 0, PQ, H * PQ)
    point_part = jnp.where(point_mask, 2.0 * weight, 0.0)
    square_part = jnp.where(point_mask, -weight, 0.0)
    q_scale = jnp.concatenate([scalar_part, point_part], 1)
    spread = jnp.concatenate(
        [
            jnp.concatenate([q_feat[i : i + 1] * q_scale, square_part], 1)
            for i in range(rows)
        ],
        0,
    )
    q_square = [
        jnp.sum(
            jnp.where(point_mask, q_feat[i : i + 1, scalar:] ** 2, 0.0), axis=1, keepdims=True
        )
        * weight
        for i in range(rows)
    ]
    bias_weights = w_bias_ref[...]

    def wait_x(step, carry):
        source = lax.rem(me + devices - step, devices)
        x_copy(source, source, step, source).wait_recv()
        return carry

    lax.fori_loop(1, devices, wait_x, 0)
    loads[2].wait()

    chunk = LANES if slots % LANES == 0 else slots

    def key_side(start):
        part = pl.ds(start, chunk)
        inputs = [x_all[part, t, :].astype(jnp.bfloat16) for t in range(CS // LANES)]
        held = x_all[part, CS // LANES, :].T
        values = lax.dot_general(
            w_keyval_ref[...],
            jnp.concatenate(inputs, 1),
            NT,
            preferred_element_type=jnp.float32,
        )
        first, second = 2 * scalar, 2 * scalar + 3 * H * PQ
        key_points = moved_columns(held, values[first:second], H * PQ)
        value_points = moved_columns(held, values[second:], H * PV)
        squares = [point * point for point in key_points]
        k_feat[:, part] = jnp.concatenate([values[:scalar]] + key_points + squares, 0)
        v_feat[:, part] = jnp.concatenate([values[scalar:first]] + value_points, 0)

    if chunk == slots:
        key_side(0)
    else:

        @pl.loop(0, slots // chunk)
        def _(index):
            key_side(pl.multiple_of(index * chunk, chunk))

    inner = dot_exact(spread, k_feat[...], NN)

    def wait_p(step, carry):
        source = lax.rem(col + col_devs - step, col_devs)
        p_copy(source, source, step, source).wait_recv()
        return carry

    lax.fori_loop(1, col_devs, wait_p, 0)

    place = lax.rem(lax.broadcasted_iota(jnp.int32, (HP, slots), 1), key_pad)
    bias_rows = jnp.concatenate([bias_weights, jnp.zeros((HP - H, CZ), jnp.float32)], 0)
    shares, pooled = [], []
    for i in range(rows):
        block = pair_all[i]
        if key_pad != keys:
            block = jnp.concatenate(
                [block, jnp.zeros((col_devs, key_pad - keys, CZ), jnp.float32)], 1
            )
        block = block.reshape(slots, CZ)
        bias = dot_exact(bias_rows, block, NT)
        logits = math.sqrt(1.0 / 3.0) * (inner[i * HP : (i + 1) * HP] + bias - q_square[i])
        if key_pad != keys:
            logits = jnp.where(place < keys, logits, -jnp.inf)
        exponent = jnp.exp(logits - jnp.max(logits, axis=1, keepdims=True))
        share = exponent / jnp.sum(exponent, axis=1, keepdims=True)
        shares.append(share)
        pooled.append(dot_exact(share, block, NN))

    gathered = dot_exact(jnp.concatenate(shares, 0), v_feat[...], NT)
    value_masks = [head_mask(scalar, 0, CH, scalar), head_mask(3 * H * PV, 0, PV, H * PV)]
    value_mask = jnp.concatenate([jnp.where(mask, 1.0, 0.0) for mask in value_masks], 1)
    kept = jnp.concatenate(
        [
            jnp.sum(
                gathered[i * HP : (i + 1) * HP] * value_mask,
                axis=0,
                keepdims=True,
            )
            for i in range(rows)
        ],
        0,
    )
    wide = H * PV
    relative = [
        kept[:, scalar + b * wide : scalar + (b + 1) * wide] - frame[:, 9 + b : 10 + b]
        for b in range(3)
    ]
    local = [
        frame[:, a : a + 1] * relative[0]
        + frame[:, 3 + a : 4 + a] * relative[1]
        + frame[:, 6 + a : 7 + a] * relative[2]
        for a in range(3)
    ]
    length = jnp.sqrt(local[0] ** 2 + local[1] ** 2 + local[2] ** 2 + 1.0)
    loads[3].wait()
    features = jnp.concatenate([kept[:, :scalar]] + local + [length], 1).astype(jnp.bfloat16)
    split = H * (CH + 4 * PV)
    total = jnp.dot(features, w_out_ref[0:split, :], preferred_element_type=jnp.float32)
    flat = jnp.concatenate(
        [
            jnp.concatenate([pooled[i][h : h + 1] for i in range(rows)], 0)
            for h in range(H)
        ],
        1,
    )
    high = flat.astype(jnp.bfloat16)
    rest = flat - high.astype(jnp.float32)
    middle = rest.astype(jnp.bfloat16)
    low = (rest - middle.astype(jnp.float32)).astype(jnp.bfloat16)
    w_pair = w_out_ref[split:, :]
    for piece in (low, middle, high):
        total = total + jnp.dot(piece, w_pair, preferred_element_type=jnp.float32)
    out_ref[...] = total

    def end_x(step, carry):
        peer = lax.rem(me + step, devices)
        x_copy(me, peer, step, me).wait_send()
        return carry

    def end_p(step, carry):
        p_copy(lax.rem(col + step, col_devs), col, step, col).wait_send()
        return carry

    lax.fori_loop(1, devices, end_x, 0)
    lax.fori_loop(1, col_devs, end_p, 0)


def solution(mesh):
    sizes = (mesh.shape["row"], mesh.shape["col"])
    devices = sizes[0] * sizes[1]

    def body(singles, pair, frames, w_query, w_keyval, w_bias, head_weights, w_out):
        rows = singles.shape[0]
        keys = pair.shape[1]
        slots = sizes[1] * round_up(keys, 8)
        vmem = pl.BlockSpec(memory_space=pltpu.VMEM)
        hbm = pl.BlockSpec(memory_space=pl.ANY)
        return pl.pallas_call(
            functools.partial(kernel, sizes),
            out_shape=jax.ShapeDtypeStruct((rows, w_out.shape[1]), jnp.float32),
            in_specs=[vmem] * 4 + [hbm] * 4,
            out_specs=vmem,
            scratch_shapes=[
                pltpu.VMEM((slots, CS // LANES + 1, LANES), jnp.float32),
                pltpu.VMEM((keys, pair.shape[0], CZ), jnp.float32),
                pltpu.VMEM(pair.shape, jnp.float32),
                pltpu.VMEM((rows, sizes[1], keys, CZ), jnp.float32),
                pltpu.VMEM(w_query.shape[::-1], w_query.dtype),
                pltpu.VMEM(w_keyval.shape[::-1], w_keyval.dtype),
                pltpu.VMEM(w_out.shape, w_out.dtype),
                pltpu.VMEM((H * CH + 6 * H * PQ, slots), jnp.float32),
                pltpu.VMEM((H * CH + 3 * H * PV, slots), jnp.float32),
                pltpu.SemaphoreType.DMA((4,)),
                pltpu.SemaphoreType.DMA((devices,)),
                pltpu.SemaphoreType.DMA((devices,)),
                pltpu.SemaphoreType.DMA((sizes[1],)),
                pltpu.SemaphoreType.DMA((sizes[1],)),
            ],
            compiler_params=pltpu.CompilerParams(
                collective_id=0, has_side_effects=True, vmem_limit_bytes=60 * 2**20
            ),
        )(
            singles,
            frames,
            w_bias.T,
            head_weights.reshape(1, H),
            pair.transpose(1, 0, 2),
            w_query.T,
            w_keyval.T,
            w_out,
        )

    return jax.shard_map(
        body,
        mesh=mesh,
        in_specs=(
            P(("row", "col"), None),
            P("row", "col", None),
            P(("row", "col"), None),
            P(),
            P(),
            P(),
            P(),
            P(),
        ),
        out_specs=P(("row", "col"), None),
        check_vma=False,
    )
```

```python
import functools
import math

import jax
import jax.numpy as jnp
from jax import lax
from jax.experimental import pallas as pl
from jax.experimental.pallas import tpu as pltpu
from jax.sharding import PartitionSpec as P

CS = 384
CZ = 128
H = 12
CH = 16
PQ = 4
PV = 8

HP = 16
LANES = 128
HIGHEST = lax.Precision.HIGHEST
MESH = pl.DeviceIdType.MESH
NT = (((1,), (1,)), ((), ()))
NN = (((1,), (0,)), ((), ()))


def round_up(value, step):
    return (value + step - 1) // step * step


def dot_exact(left, right, dims):
    return lax.dot_general(
        left, right, dims, precision=HIGHEST, preferred_element_type=jnp.float32
    )


def head_mask(width, offset, per_head, heads_period):
    feature = lax.broadcasted_iota(jnp.int32, (HP, width), 1) - offset
    head = lax.broadcasted_iota(jnp.int32, (HP, width), 0)
    return (feature % heads_period) // per_head == head


def moved_points(frame, local, width):
    parts = [local[:, b * width : (b + 1) * width] for b in range(3)]
    return [
        frame[:, 3 * a : 3 * a + 1] * parts[0]
        + frame[:, 3 * a + 1 : 3 * a + 2] * parts[1]
        + frame[:, 3 * a + 2 : 3 * a + 3] * parts[2]
        + frame[:, 9 + a : 10 + a]
        for a in range(3)
    ]


def moved_columns(frame, local, width):
    parts = [local[b * width : (b + 1) * width] for b in range(3)]
    return [
        frame[3 * a : 3 * a + 1] * parts[0]
        + frame[3 * a + 1 : 3 * a + 2] * parts[1]
        + frame[3 * a + 2 : 3 * a + 3] * parts[2]
        + frame[9 + a : 10 + a]
        for a in range(3)
    ]


def kernel(
    sizes,
    singles_ref,
    frames_ref,
    w_bias_ref,
    heads_ref,
    pair_hbm,
    w_query_hbm,
    w_keyval_hbm,
    w_out_hbm,
    out_ref,
    x_all,
    pair_raw,
    pair_own,
    pair_all,
    w_query_ref,
    w_keyval_ref,
    w_out_ref,
    k_feat,
    v_feat,
    load_sem,
    x_send,
    x_recv,
    p_send,
    p_recv,
):
    row_devs, col_devs = sizes
    devices = row_devs * col_devs
    rows = singles_ref.shape[0]
    keys = pair_own.shape[1]
    key_pad = round_up(keys, 8)
    slots = col_devs * key_pad
    row = lax.axis_index("row")
    col = lax.axis_index("col")
    me = row * col_devs + col

    loads = [
        pltpu.make_async_copy(pair_hbm, pair_raw, load_sem.at[0]),
        pltpu.make_async_copy(w_query_hbm, w_query_ref, load_sem.at[1]),
        pltpu.make_async_copy(w_keyval_hbm, w_keyval_ref, load_sem.at[2]),
        pltpu.make_async_copy(w_out_hbm, w_out_ref, load_sem.at[3]),
    ]
    for load in loads:
        load.start()

    barrier = pltpu.get_barrier_semaphore()
    core = lax.rem(row, 2)
    place_in_plane = row // 2 * col_devs + col
    plane = devices // 2

    def in_plane(step):
        index = lax.rem(place_in_plane + step, plane)
        return (index // col_devs * 2 + core, lax.rem(index, col_devs))

    def partner_of(peer):
        return (peer[0] // 2 * 2 + 1 - lax.rem(peer[0], 2), peer[1])

    def number_of(peer):
        return peer[0] * col_devs + peer[1]

    here = (row, col)

    def greet_one(peer):
        pl.semaphore_signal(barrier, inc=1, device_id=peer, device_id_type=MESH)

    def greet(step, carry):
        greet_one(in_plane(step))
        return carry

    lax.fori_loop(1, plane, greet, 0)
    greet_one(partner_of(here))

    def slot_of(device):
        first = device * rows
        return first // keys * key_pad + lax.rem(first, keys)

    for c in range(col_devs):
        for slot in range(c * key_pad + keys, (c + 1) * key_pad):
            x_all[slot] = jnp.zeros(x_all.shape[1:], jnp.float32)
    single = singles_ref[...]
    frame = frames_ref[...]
    own_slot = pl.ds(slot_of(me), rows)
    for t in range(CS // LANES):
        x_all[own_slot, t, :] = single[:, t * LANES : (t + 1) * LANES].astype(jnp.float32)
    x_all[own_slot, CS // LANES, :] = jnp.concatenate(
        [frame, jnp.zeros((rows, LANES - 12), jnp.float32)], 1
    )
    loads[0].wait()
    for i in range(pair_own.shape[0]):
        pair_own[i] = pair_raw[:, i, :]
    for i in range(rows):
        pair_all[i, col] = pair_own[col * rows + i]
    pl.semaphore_wait(barrier, plane)

    def x_copy(source, peer, send_index):
        number = number_of(source)
        slot = pl.ds(slot_of(number), rows)
        return pltpu.make_async_remote_copy(
            src_ref=x_all.at[slot],
            dst_ref=x_all.at[slot],
            send_sem=x_send.at[send_index],
            recv_sem=x_recv.at[number],
            device_id=peer,
            device_id_type=MESH,
        )

    def x_direct(step):
        peer = in_plane(step)
        return x_copy(here, peer, number_of(peer))

    def x_relay(source):
        return x_copy(source, partner_of(here), number_of(partner_of(source)))

    def p_copy(peer_col, sent_col, send_index, recv_index):
        return pltpu.make_async_remote_copy(
            src_ref=pair_own.at[pl.ds(peer_col * rows, rows)],
            dst_ref=pair_all.at[:, sent_col],
            send_sem=p_send.at[send_index],
            recv_sem=p_recv.at[recv_index],
            device_id=(row, peer_col),
            device_id_type=MESH,
        )

    def send_x(step, carry):
        x_direct(step).start()
        return carry

    def send_p(step, carry):
        p_copy(lax.rem(col + step, col_devs), col, step, col).start()
        return carry

    lax.fori_loop(1, plane, send_x, 0)
    x_relay(here).start()
    lax.fori_loop(1, col_devs, send_p, 0)

    scalar = H * CH
    loads[1].wait()
    projected = lax.dot_general(
        single, w_query_ref[...], NT, preferred_element_type=jnp.float32
    )
    q_points = moved_points(frame, projected[:, scalar:], H * PQ)
    q_feat = jnp.concatenate([projected[:, :scalar]] + q_points, 1)

    raw = heads_ref[...]
    gamma_row = jnp.maximum(raw, 0.0) + jnp.log(1.0 + jnp.exp(-jnp.abs(raw)))
    eye = lax.broadcasted_iota(jnp.int32, (HP, H), 0) == lax.broadcasted_iota(
        jnp.int32, (HP, H), 1
    )
    gamma = jnp.sum(jnp.where(eye, gamma_row, 0.0), axis=1, keepdims=True)
    weight = gamma * (math.sqrt(2.0 / (9.0 * PQ)) / 2.0)
    scalar_part = jnp.where(head_mask(scalar, 0, CH, scalar), 1.0 / math.sqrt(CH), 0.0)
    point_mask = head_mask(3 * H * PQ, 0, PQ, H * PQ)
    point_part = jnp.where(point_mask, 2.0 * weight, 0.0)
    square_part = jnp.where(point_mask, -weight, 0.0)
    q_scale = jnp.concatenate([scalar_part, point_part], 1)
    spread = jnp.concatenate(
        [
            jnp.concatenate([q_feat[i : i + 1] * q_scale, square_part], 1)
            for i in range(rows)
        ],
        0,
    )
    q_square = [
        jnp.sum(
            jnp.where(point_mask, q_feat[i : i + 1, scalar:] ** 2, 0.0), axis=1, keepdims=True
        )
        * weight
        for i in range(rows)
    ]
    bias_weights = w_bias_ref[...]

    def pass_on(step, carry):
        source = in_plane(plane - step)
        x_relay(source).wait_recv()
        x_relay(source).start()
        return carry

    def wait_x(step, carry):
        x_relay(partner_of(in_plane(plane - step))).wait_recv()
        return carry

    lax.fori_loop(1, plane, pass_on, 0)
    lax.fori_loop(0, plane, wait_x, 0)
    loads[2].wait()

    chunk = LANES if slots % LANES == 0 else slots

    def key_side(start):
        part = pl.ds(start, chunk)
        inputs = [x_all[part, t, :].astype(jnp.bfloat16) for t in range(CS // LANES)]
        held = x_all[part, CS // LANES, :].T
        values = lax.dot_general(
            w_keyval_ref[...],
            jnp.concatenate(inputs, 1),
            NT,
            preferred_element_type=jnp.float32,
        )
        first, second = 2 * scalar, 2 * scalar + 3 * H * PQ
        key_points = moved_columns(held, values[first:second], H * PQ)
        value_points = moved_columns(held, values[second:], H * PV)
        squares = [point * point for point in key_points]
        k_feat[:, part] = jnp.concatenate([values[:scalar]] + key_points + squares, 0)
        v_feat[:, part] = jnp.concatenate([values[scalar:first]] + value_points, 0)

    if chunk == slots:
        key_side(0)
    else:

        @pl.loop(0, slots // chunk)
        def _(index):
            key_side(pl.multiple_of(index * chunk, chunk))

    inner = dot_exact(spread, k_feat[...], NN)

    def wait_p(step, carry):
        source = lax.rem(col + col_devs - step, col_devs)
        p_copy(source, source, step, source).wait_recv()
        return carry

    lax.fori_loop(1, col_devs, wait_p, 0)

    place = lax.rem(lax.broadcasted_iota(jnp.int32, (HP, slots), 1), key_pad)
    bias_rows = jnp.concatenate([bias_weights, jnp.zeros((HP - H, CZ), jnp.float32)], 0)
    shares, pooled = [], []
    for i in range(rows):
        block = pair_all[i]
        if key_pad != keys:
            block = jnp.concatenate(
                [block, jnp.zeros((col_devs, key_pad - keys, CZ), jnp.float32)], 1
            )
        block = block.reshape(slots, CZ)
        bias = dot_exact(bias_rows, block, NT)
        logits = math.sqrt(1.0 / 3.0) * (inner[i * HP : (i + 1) * HP] + bias - q_square[i])
        if key_pad != keys:
            logits = jnp.where(place < keys, logits, -jnp.inf)
        exponent = jnp.exp(logits - jnp.max(logits, axis=1, keepdims=True))
        share = exponent / jnp.sum(exponent, axis=1, keepdims=True)
        shares.append(share)
        pooled.append(dot_exact(share, block, NN))

    gathered = dot_exact(jnp.concatenate(shares, 0), v_feat[...], NT)
    value_masks = [head_mask(scalar, 0, CH, scalar), head_mask(3 * H * PV, 0, PV, H * PV)]
    value_mask = jnp.concatenate([jnp.where(mask, 1.0, 0.0) for mask in value_masks], 1)
    kept = jnp.concatenate(
        [
            jnp.sum(
                gathered[i * HP : (i + 1) * HP] * value_mask,
                axis=0,
                keepdims=True,
            )
            for i in range(rows)
        ],
        0,
    )
    wide = H * PV
    relative = [
        kept[:, scalar + b * wide : scalar + (b + 1) * wide] - frame[:, 9 + b : 10 + b]
        for b in range(3)
    ]
    local = [
        frame[:, a : a + 1] * relative[0]
        + frame[:, 3 + a : 4 + a] * relative[1]
        + frame[:, 6 + a : 7 + a] * relative[2]
        for a in range(3)
    ]
    length = jnp.sqrt(local[0] ** 2 + local[1] ** 2 + local[2] ** 2 + 1.0)
    loads[3].wait()
    features = jnp.concatenate([kept[:, :scalar]] + local + [length], 1).astype(jnp.bfloat16)
    split = H * (CH + 4 * PV)
    total = jnp.dot(features, w_out_ref[0:split, :], preferred_element_type=jnp.float32)
    flat = jnp.concatenate(
        [
            jnp.concatenate([pooled[i][h : h + 1] for i in range(rows)], 0)
            for h in range(H)
        ],
        1,
    )
    high = flat.astype(jnp.bfloat16)
    rest = flat - high.astype(jnp.float32)
    middle = rest.astype(jnp.bfloat16)
    low = (rest - middle.astype(jnp.float32)).astype(jnp.bfloat16)
    w_pair = w_out_ref[split:, :]
    for piece in (low, middle, high):
        total = total + jnp.dot(piece, w_pair, preferred_element_type=jnp.float32)
    out_ref[...] = total

    def end_x(step, carry):
        x_direct(step).wait_send()
        x_relay(in_plane(step)).wait_send()
        return carry

    def end_p(step, carry):
        p_copy(lax.rem(col + step, col_devs), col, step, col).wait_send()
        return carry

    x_relay(here).wait_send()
    lax.fori_loop(1, plane, end_x, 0)
    lax.fori_loop(1, col_devs, end_p, 0)


def solution(mesh):
    sizes = (mesh.shape["row"], mesh.shape["col"])
    devices = sizes[0] * sizes[1]

    def body(singles, pair, frames, w_query, w_keyval, w_bias, head_weights, w_out):
        rows = singles.shape[0]
        keys = pair.shape[1]
        slots = sizes[1] * round_up(keys, 8)
        vmem = pl.BlockSpec(memory_space=pltpu.VMEM)
        hbm = pl.BlockSpec(memory_space=pl.ANY)
        return pl.pallas_call(
            functools.partial(kernel, sizes),
            out_shape=jax.ShapeDtypeStruct((rows, w_out.shape[1]), jnp.float32),
            in_specs=[vmem] * 4 + [hbm] * 4,
            out_specs=vmem,
            scratch_shapes=[
                pltpu.VMEM((slots, CS // LANES + 1, LANES), jnp.float32),
                pltpu.VMEM((keys, pair.shape[0], CZ), jnp.float32),
                pltpu.VMEM(pair.shape, jnp.float32),
                pltpu.VMEM((rows, sizes[1], keys, CZ), jnp.float32),
                pltpu.VMEM(w_query.shape[::-1], w_query.dtype),
                pltpu.VMEM(w_keyval.shape[::-1], w_keyval.dtype),
                pltpu.VMEM(w_out.shape, w_out.dtype),
                pltpu.VMEM((H * CH + 6 * H * PQ, slots), jnp.float32),
                pltpu.VMEM((H * CH + 3 * H * PV, slots), jnp.float32),
                pltpu.SemaphoreType.DMA((4,)),
                pltpu.SemaphoreType.DMA((devices,)),
                pltpu.SemaphoreType.DMA((devices,)),
                pltpu.SemaphoreType.DMA((sizes[1],)),
                pltpu.SemaphoreType.DMA((sizes[1],)),
            ],
            compiler_params=pltpu.CompilerParams(
                collective_id=0, has_side_effects=True, vmem_limit_bytes=60 * 2**20
            ),
        )(
            singles,
            frames,
            w_bias.T,
            head_weights.reshape(1, H),
            pair.transpose(1, 0, 2),
            w_query.T,
            w_keyval.T,
            w_out,
        )

    return jax.shard_map(
        body,
        mesh=mesh,
        in_specs=(
            P(("row", "col"), None),
            P("row", "col", None),
            P(("row", "col"), None),
            P(),
            P(),
            P(),
            P(),
            P(),
        ),
        out_specs=P(("row", "col"), None),
        check_vma=False,
    )
```
